32 devices in a mesh: band: 8 (over z, x), sub: 4 (over y, core).
Axes of the slice: x: 2, y: 2, z: 4, core: 2. Of those that a mesh axis runs over, the one named last changes fastest.
Arguments:
- grad_pred: bfloat16 [227, 24576], P(None, ('band', 'sub')), may hold values from -6 to 6
- grid_latent: bfloat16 [24576, 512], P(('band', 'sub')), may hold values from -6 to 6
- mesh_latent: bfloat16 [10240, 512], P(('band', 'sub')), may hold values from -6 to 6
- send_slot: int32 [24576], P(('band', 'sub')), may hold values from 0 to 2303, as said below
- edge_src: int32 [3, 73728], P(None, ('band', 'sub')), may hold values from 0 to 10239, as said below
- w_mesh: bfloat16 [512, 512], replicated, may hold values from -0.25 to 0.25
- w_grid: bfloat16 [512, 512], replicated, may hold values from -0.25 to 0.25
- w_msg: bfloat16 [512, 512], replicated, may hold values from -0.25 to 0.25
- w_out: bfloat16 [512, 227], replicated, may hold values from -0.25 to 0.25
Outputs:
- mesh_grad: bfloat16 [10240, 512], P(('band', 'sub'))
- grad_w_mesh: float32 [512, 512], replicated
- grad_w_grid: float32 [512, 512], replicated
- grad_w_msg: float32 [512, 512], replicated
- grad_w_out: float32 [512, 227], replicated
The draws below stay inside these ranges and needn't reach their ends.
Inputs may be any that keep to these rules, and one draw needn't show every extreme that they name: For grid point p on latitude-major device i, send_slot[p] = j * 72 + r names patch-major device j and a rank r. On one device i the values are distinct, and for each j the ranks used are 0 to the count of i's points sent to j minus 1. Every such count is at most 72, and 72 is reached in every draw. Every grid point thereby gets one patch-major slot; live slots of each source stand at the front of its block of 72. One patch-major device holds at most 1920 live slots, reached on some device in every draw. `edge_src`: A slot on patch-major device j, of band b = j // 4, names senders in patch b only: mesh rows b * 1280 to (b + 1) * 1280 - 1. Entries of empty slots lie in that range too and are not read.
All inputs are finite; a program needn't handle non-finite values.
Results may differ from the reference program's by a relative error of at most 0.0076.
Values may be sent and summed in bfloat16 or wider, within the bound.
No kernel may reach another device: no remote copies, remote signals or barrier semaphores. Data moves between devices by JAX's collectives and lax.ppermute only.
A program may use at most 128 MiB of HBM per device.

```python
import math
import jax
import jax.numpy as jnp

D = 512
C = 227
G_DEV = 768
GRID = 24576
MESH = 10240
PATCH = 1280
CAP = 72
SLOT_DEV = 2304
SLOTS = 73728
N_BAND = 8
N_SUB = 4
DEVICES = 32


def relay_table(key):
    base_count = G_DEV // DEVICES
    half_base = base_count // 2
    receivers = jnp.arange(DEVICES, dtype=jnp.int32)
    band_index = receivers // N_SUB
    polar_band = (band_index < N_BAND // 8) | (band_index >= N_BAND - N_BAND // 8)
    receive_load = jnp.where(polar_band, 5 * half_base, half_base).astype(jnp.int32)
    draw_key, shuffle_key = jax.random.split(jax.random.fold_in(key, 7))
    increments = jax.random.randint(draw_key, (DEVICES,), 0, half_base + 1)
    increments = increments.at[0].set(half_base).at[DEVICES - 1].set(0)
    offsets = (increments - jnp.roll(increments, 1)).astype(jnp.int32)
    senders = jnp.arange(DEVICES, dtype=jnp.int32)
    counts = receive_load[None, :] + offsets[(receivers[None, :] - senders[:, None]) % DEVICES]
    block_ends = jnp.cumsum(counts, axis=1)
    starts = block_ends - counts
    positions = jnp.arange(G_DEV, dtype=jnp.int32)

    def one_sender(row_ends, row_starts, sub_key):
        target = jnp.sum((row_ends[None, :] <= positions[:, None]).astype(jnp.int32), axis=1)
        slot_rank = positions - row_starts[target]
        shuffle = jax.random.permutation(sub_key, G_DEV)
        return jnp.zeros((G_DEV,), jnp.int32).at[shuffle].set(target * CAP + slot_rank)
    sender_keys = jax.random.split(shuffle_key, DEVICES)
    table = jax.vmap(one_sender)(block_ends, starts, sender_keys)
    return table.reshape(GRID).astype(jnp.int32)


def draw_send_slot(key, part):
    return relay_table(key)


def draw_edge_src(key, part):
    local_node = jax.random.randint(jax.random.fold_in(key, 11), (3, SLOTS), 0, PATCH)
    holders = jnp.arange(SLOTS, dtype=jnp.int32) // SLOT_DEV
    band_index = holders // N_SUB
    return (local_node + band_index[None, :] * PATCH).astype(jnp.int32)


def steps_of(rng, shape, cuts, low, largest):
    def one(dim, blocks):
        steps = jax.random.uniform(jax.random.fold_in(jax.random.fold_in(rng, 6), dim), (blocks,), jnp.float32, low / len(cuts), largest / len(cuts))
        return jnp.repeat(jnp.exp(steps), shape[dim] // blocks).reshape((-1,) + (1,) * (len(shape) - dim - 1))

    loudness = one(*cuts[0])
    for cut in cuts[1:]:
        loudness = loudness * one(*cut)
    return loudness


def bell_draw(rng, dims, scale, bound, cuts=(), kind=jnp.bfloat16):
    factor_of = steps_of(rng, dims, cuts, -0.22, 0.18) if cuts else 1.0
    values = jax.random.normal(rng, dims, jnp.float32) * scale * factor_of
    return jnp.minimum(jnp.maximum(values, -bound), bound).astype(kind)


def setup_inputs(seed: int = 0) -> dict:
    seeds = jax.random.split(jax.random.key(seed), 10)
    grad_pred = bell_draw(seeds[0], (C, GRID), 1.0, 6.0, ((1, 32),))
    grid_latent = bell_draw(seeds[1], (GRID, D), 1.0, 6.0, ((0, 32),))
    mesh_latent = bell_draw(seeds[2], (MESH, D), 1.0, 6.0, ((0, 32),))
    send_slot = draw_send_slot(jax.random.fold_in(seeds[9], 71), 0)
    edge_src = draw_edge_src(jax.random.fold_in(seeds[9], 71), 0)
    w_mesh = bell_draw(seeds[5], (D, D), D ** -0.5, 0.25)
    w_grid = bell_draw(seeds[6], (D, D), D ** -0.5, 0.25)
    w_msg = bell_draw(seeds[7], (D, D), D ** -0.5, 0.25)
    w_out = bell_draw(seeds[8], (D, C), D ** -0.5, 0.25)
    return {"grad_pred": grad_pred, "grid_latent": grid_latent, "mesh_latent": mesh_latent, "send_slot": send_slot, "edge_src": edge_src, "w_mesh": w_mesh, "w_grid": w_grid, "w_msg": w_msg, "w_out": w_out}


def latitude_weight(points, total):
    angle = jnp.pi * ((points.astype(jnp.float32) + 0.5) / total - 0.5)
    return 0.5 * jnp.pi * jnp.cos(angle)

def silu_slope(value):
    sigma = jax.nn.sigmoid(value)
    return sigma * (1.0 + value * (1.0 - sigma))

def reference(grad_pred, grid_latent, mesh_latent, send_slot, edge_src, w_mesh, w_grid, w_msg, w_out):
    points = jnp.arange(GRID, dtype=jnp.int32)
    source_dev = (points // G_DEV).astype(jnp.int32)
    target = (send_slot // CAP).astype(jnp.int32)
    slot_rank = (send_slot % CAP).astype(jnp.int32)
    holder = (target * SLOT_DEV + source_dev * CAP + slot_rank).astype(jnp.int32)
    senders = edge_src[:, holder]
    grid_proj = jnp.dot(grid_latent, w_grid, preferred_element_type=jnp.float32).astype(jnp.bfloat16)
    mesh_proj = jnp.dot(mesh_latent, w_mesh, preferred_element_type=jnp.float32).astype(jnp.bfloat16)
    grid_float = grid_proj.astype(jnp.float32)
    pre_acts = [mesh_proj[senders[corner]].astype(jnp.float32) + grid_float for corner in range(3)]
    act_sum = (jax.nn.silu(pre_acts[0]) + jax.nn.silu(pre_acts[1]) + jax.nn.silu(pre_acts[2])).astype(jnp.bfloat16)
    aggregate = jnp.dot(act_sum, w_msg, preferred_element_type=jnp.float32).astype(jnp.bfloat16)
    weighted = (latitude_weight(points, GRID)[None, :] * grad_pred.astype(jnp.float32)).astype(jnp.bfloat16)
    raw_out = jnp.dot(aggregate.T, weighted.T, preferred_element_type=jnp.float32)
    agg_grad = jnp.dot(weighted.T, w_out.T, preferred_element_type=jnp.float32).astype(jnp.bfloat16)
    raw_msg = jnp.dot(act_sum.T, agg_grad, preferred_element_type=jnp.float32)
    act_grad = jnp.dot(agg_grad, w_msg.T, preferred_element_type=jnp.float32)
    pre_grads = [(act_grad * silu_slope(pre)).astype(jnp.bfloat16) for pre in pre_acts]
    grid_proj_grad = (pre_grads[0].astype(jnp.float32) + pre_grads[1].astype(jnp.float32) + pre_grads[2].astype(jnp.float32)).astype(jnp.bfloat16)
    raw_grid = jnp.dot(grid_latent.T, grid_proj_grad, preferred_element_type=jnp.float32)
    node_total = jnp.zeros((MESH, D), jnp.float32)
    for corner in range(3):
        node_total = node_total.at[senders[corner]].add(pre_grads[corner].astype(jnp.float32))
    mesh_proj_grad = node_total.astype(jnp.bfloat16)
    mesh_grad = jnp.dot(mesh_proj_grad, w_mesh.T, preferred_element_type=jnp.float32).astype(jnp.bfloat16)
    raw_mesh = jnp.dot(mesh_latent.T, mesh_proj_grad, preferred_element_type=jnp.float32)
    grad_scale = 1.0 / math.sqrt(3.0 * GRID)
    return (mesh_grad, raw_mesh * grad_scale, raw_grid * grad_scale, raw_msg * grad_scale, raw_out * grad_scale)
```

```python
import functools
import math

import jax
import jax.numpy as jnp
from jax import lax
from jax.experimental import pallas as pl
from jax.experimental.pallas import tpu as pltpu
from jax.sharding import PartitionSpec as P

CHUNKS = 3
LANES = 128


def latitude_weight(points, total):
    angle = jnp.pi * ((points.astype(jnp.float32) + 0.5) / total - 0.5)
    return 0.5 * jnp.pi * jnp.cos(angle)


def dot(left, right, left_dim, right_dim):
    return lax.dot_general(
        left, right, (((left_dim,), (right_dim,)), ((), ())), preferred_element_type=jnp.float32
    )


def one_hot(index, dim, size):
    shape = (index.shape[0], size) if dim == 1 else (size, index.shape[1])
    return jnp.where(lax.broadcasted_iota(jnp.int32, shape, dim) == index, 1.0, 0.0).astype(
        jnp.bfloat16
    )


def row_block(rows):
    for block in (256, 128, 64, 32, 16, 8):
        if rows % block == 0:
            return block
    return rows


def pack_body(place, latent, weighted, out, *, block, width, base):
    first = base + pl.program_id(0) * block
    select = one_hot(place[...] - first, 0, block)
    out[:, :width] = dot(select, latent[...], 1, 0).astype(jnp.bfloat16)
    out[:, width:] = dot(select, weighted[...], 1, 1).astype(jnp.bfloat16)


def pack(place, latent, weighted, base, rows):
    width = latent.shape[1]
    extra = weighted.shape[0]
    block = row_block(rows)
    whole = lambda array: pl.BlockSpec(array.shape, lambda i: (0,) * array.ndim)
    return pl.pallas_call(
        functools.partial(pack_body, block=block, width=width, base=base),
        grid=(rows // block,),
        in_specs=[whole(place), whole(latent), whole(weighted)],
        out_specs=pl.BlockSpec((block, width + extra), lambda i: (i, 0)),
        out_shape=jax.ShapeDtypeStruct((rows, width + extra), jnp.bfloat16),
        cost_estimate=pl.CostEstimate(
            flops=2 * rows * latent.shape[0] * (width + extra),
            bytes_accessed=rows * (width + extra) * 4,
            transcendentals=0,
        ),
        name="pack",
    )(place, latent, weighted)


def edge_body(*refs, width, chained):
    rows_in, columns, lanes, table, w_grid, w_both = refs[:6]
    outer, grid_part, node_part = refs[-3:]

    @pl.when(pl.program_id(0) == 0)
    def _():
        if chained:
            for old, new in zip(refs[6:9], refs[-3:]):
                new[...] = old[...]
        else:
            for new in refs[-3:]:
                new[...] = jnp.zeros_like(new)

    latent = rows_in[:, :width]
    weighted = rows_in[:, width:]
    nodes = table.shape[0]
    grid_proj = dot(latent, w_grid[...], 1, 0).astype(jnp.bfloat16).astype(jnp.float32)
    act_grad = dot(weighted, w_both[...], 1, 1)
    act_sum = None
    proj_grad = None
    node_sum = None
    for corner in range(3):
        gathered = dot(one_hot(columns[:, corner : corner + 1], 1, nodes), table[...], 1, 0)
        pre = gathered + grid_proj
        sigma = 0.5 * jnp.tanh(0.5 * pre) + 0.5
        act = pre * sigma
        grad = (act_grad * (sigma + act * (1.0 - sigma))).astype(jnp.bfloat16)
        spread = dot(one_hot(lanes[corner : corner + 1, :], 0, nodes), grad, 1, 0)
        wide = grad.astype(jnp.float32)
        act_sum = act if act_sum is None else act_sum + act
        proj_grad = wide if proj_grad is None else proj_grad + wide
        node_sum = spread if node_sum is None else node_sum + spread
    node_part[...] += node_sum
    outer[...] += dot(weighted, act_sum.astype(jnp.bfloat16), 0, 0)
    grid_part[...] += dot(latent, proj_grad.astype(jnp.bfloat16), 0, 0)


def edges(rows_in, columns, lanes, table, w_grid, w_both, previous):
    rows, row_width = rows_in.shape
    nodes, width = table.shape
    extra = row_width - width
    block = row_block(rows)
    whole = lambda shape: pl.BlockSpec(shape, lambda i: (0,) * len(shape))
    shapes = ((extra, width), (width, width), (nodes, width))
    chained = previous is not None
    in_specs = [
        pl.BlockSpec((block, row_width), lambda i: (i, 0)),
        pl.BlockSpec((block, columns.shape[1]), lambda i: (i, 0)),
        pl.BlockSpec((lanes.shape[0], block), lambda i: (0, i)),
        whole(table.shape),
        whole(w_grid.shape),
        whole(w_both.shape),
    ]
    operands = [rows_in, columns, lanes, table, w_grid, w_both]
    if chained:
        in_specs += [whole(shape) for shape in shapes]
        operands += list(previous)
    return pl.pallas_call(
        functools.partial(edge_body, width=width, chained=chained),
        grid=(rows // block,),
        in_specs=in_specs,
        out_specs=[whole(shape) for shape in shapes],
        out_shape=[jax.ShapeDtypeStruct(shape, jnp.float32) for shape in shapes],
        compiler_params=pltpu.CompilerParams(vmem_limit_bytes=56 * 1024 * 1024),
        cost_estimate=pl.CostEstimate(
            flops=2 * rows * width * (6 * nodes + 2 * width + 2 * extra),
            bytes_accessed=rows * row_width * 2 + 4 * nodes * width * 4,
            transcendentals=3 * rows * width,
        ),
        name="edges",
    )(*operands)


def shards(grad_pred, grid_latent, mesh_latent, send_slot, edge_src, w_mesh, w_grid, w_msg, w_out):
    grid_rows, width = grid_latent.shape
    channels = grad_pred.shape[0]
    axes = ("band", "sub")
    devices = lax.axis_size(axes)
    members = lax.axis_size("sub")
    capacity = 3 * grid_rows // devices
    total_points = grid_rows * devices
    extra = -(-channels // LANES) * LANES
    step = capacity // CHUNKS
    chunk_rows = devices * step

    patch_latent = lax.all_gather(mesh_latent, "sub", axis=0, tiled=True)
    patch_size = patch_latent.shape[0]

    points = lax.axis_index(axes) * grid_rows + jnp.arange(grid_rows, dtype=jnp.int32)
    weighted = (
        latitude_weight(points, total_points)[None, :] * grad_pred.astype(jnp.float32)
    ).astype(jnp.bfloat16)
    weighted = jnp.pad(weighted, ((0, extra - channels), (0, 0)))
    target = send_slot // capacity
    rank = send_slot % capacity
    place = (rank // step) * chunk_rows + target * step + rank % step
    place = place[None, :]
    arrived = []
    for chunk in range(CHUNKS):
        packed = pack(place, grid_latent, weighted, chunk * chunk_rows, chunk_rows)
        received = lax.all_to_all(
            packed.reshape(devices, step, width + extra), axes, split_axis=0, concat_axis=0, tiled=True
        )
        arrived.append(received.reshape(chunk_rows, width + extra))

    local = edge_src - lax.axis_index("band") * patch_size
    local = local.reshape(3, devices, CHUNKS, step).transpose(2, 0, 1, 3)
    local = local.reshape(CHUNKS, 3, chunk_rows)
    local_columns = local.transpose(0, 2, 1)
    w_both = jnp.pad(
        dot(w_msg, w_out, 1, 0).astype(jnp.bfloat16), ((0, 0), (0, extra - channels))
    )
    table = dot(patch_latent, w_mesh, 1, 0).astype(jnp.bfloat16)
    sums = None
    for chunk in range(CHUNKS):
        sums = edges(
            arrived[chunk], local_columns[chunk], local[chunk], table, w_grid, w_both, sums
        )
    outer_part, grid_part, node_part = sums

    node_sent = node_part.astype(jnp.bfloat16)
    mesh_part = dot(patch_latent, node_sent, 0, 0)
    node_blocks = lax.all_to_all(
        node_sent.reshape(members, patch_size // members, width),
        "sub",
        split_axis=0,
        concat_axis=0,
        tiled=True,
    )
    outer_total, grid_total, mesh_total = lax.psum(
        (
            outer_part.astype(jnp.bfloat16),
            grid_part.astype(jnp.bfloat16),
            mesh_part.astype(jnp.bfloat16),
        ),
        axes,
    )
    mesh_proj_grad = jnp.sum(node_blocks.astype(jnp.float32), axis=0).astype(jnp.bfloat16)
    mesh_grad = dot(mesh_proj_grad, w_mesh, 1, 1).astype(jnp.bfloat16)
    grad_scale = 1.0 / math.sqrt(3.0 * total_points)
    outer_total = outer_total[:channels]
    out_total = dot(w_msg, outer_total, 0, 1)
    msg_total = dot(outer_total, w_out, 0, 1)
    return (
        mesh_grad,
        mesh_total.astype(jnp.float32) * grad_scale,
        grid_total.astype(jnp.float32) * grad_scale,
        msg_total * grad_scale,
        out_total * grad_scale,
    )


def solution(mesh):
    placed = (
        P(None, ("band", "sub")),
        P(("band", "sub"), None),
        P(("band", "sub"), None),
        P(("band", "sub")),
        P(None, ("band", "sub")),
        P(),
        P(),
        P(),
        P(),
    )
    return jax.shard_map(
        shards,
        mesh=mesh,
        in_specs=placed,
        out_specs=(P(("band", "sub"), None), P(), P(), P(), P()),
        check_vma=False,
    )
```

```python
import functools
import math

import jax
import jax.numpy as jnp
from jax import lax
from jax.experimental import pallas as pl
from jax.experimental.pallas import tpu as pltpu
from jax.sharding import PartitionSpec as P

CHUNKS = 3
LANES = 128


def latitude_weight(points, total):
    angle = jnp.pi * ((points.astype(jnp.float32) + 0.5) / total - 0.5)
    return 0.5 * jnp.pi * jnp.cos(angle)


def dot(left, right, left_dim, right_dim):
    return lax.dot_general(
        left, right, (((left_dim,), (right_dim,)), ((), ())), preferred_element_type=jnp.float32
    )


def one_hot(index, dim, size):
    shape = (index.shape[0], size) if dim == 1 else (size, index.shape[1])
    return jnp.where(lax.broadcasted_iota(jnp.int32, shape, dim) == index, 1.0, 0.0).astype(
        jnp.bfloat16
    )


def row_block(rows):
    for block in (256, 128, 64, 32, 16, 8):
        if rows % block == 0:
            return block
    return rows


def pack_body(place, latent, weighted, *rest, block, width, base):
    out = rest[-1]
    first = base + pl.program_id(0) * block
    select = one_hot(place[...] - first, 0, block)
    out[:, :width] = dot(select, latent[...], 1, 0).astype(jnp.bfloat16)
    out[:, width:] = dot(select, weighted[...], 1, 1).astype(jnp.bfloat16)


def pack(place, latent, weighted, base, rows, after):
    width = latent.shape[1]
    extra = weighted.shape[0]
    block = row_block(rows)
    whole = lambda array: pl.BlockSpec(array.shape, lambda i: (0,) * array.ndim)
    in_specs = [whole(place), whole(latent), whole(weighted)]
    operands = [place, latent, weighted]
    if after is not None:
        in_specs.append(pl.BlockSpec((8, LANES), lambda i: (0, 0)))
        operands.append(after)
    return pl.pallas_call(
        functools.partial(pack_body, block=block, width=width, base=base),
        grid=(rows // block,),
        in_specs=in_specs,
        out_specs=pl.BlockSpec((block, width + extra), lambda i: (i, 0)),
        out_shape=jax.ShapeDtypeStruct((rows, width + extra), jnp.bfloat16),
        cost_estimate=pl.CostEstimate(
            flops=2 * rows * latent.shape[0] * (width + extra),
            bytes_accessed=rows * (width + extra) * 4,
            transcendentals=0,
        ),
        name="pack",
    )(*operands)


def edge_body(*refs, width, chained, last):
    rows_in, columns, lanes, table, w_grid, w_both = refs[:6]
    sums = refs[-3:]
    outer, grid_part, node_part = sums

    @pl.when(pl.program_id(0) == 0)
    def _():
        if chained:
            for old, new in zip(refs[6:9], sums):
                new[...] = old[...]
        else:
            for new in sums:
                new[...] = jnp.zeros_like(new)

    latent = rows_in[:, :width]
    weighted = rows_in[:, width:]
    nodes = table.shape[0]
    grid_proj = dot(latent, w_grid[...], 1, 0).astype(jnp.bfloat16).astype(jnp.float32)
    act_grad = dot(weighted, w_both[...], 1, 1)
    act_sum = None
    proj_grad = None
    node_sum = None
    for corner in range(3):
        gathered = dot(one_hot(columns[:, corner : corner + 1], 1, nodes), table[...], 1, 0)
        pre = gathered + grid_proj
        sigma = 0.5 * jnp.tanh(0.5 * pre) + 0.5
        act = pre * sigma
        grad = (act_grad * (sigma + act * (1.0 - sigma))).astype(jnp.bfloat16)
        spread = dot(one_hot(lanes[corner : corner + 1, :], 0, nodes), grad, 1, 0)
        wide = grad.astype(jnp.float32)
        act_sum = act if act_sum is None else act_sum + act
        proj_grad = wide if proj_grad is None else proj_grad + wide
        node_sum = spread if node_sum is None else node_sum + spread
    node_part[...] += node_sum
    outer[...] += dot(weighted, act_sum.astype(jnp.bfloat16), 0, 0)
    grid_part[...] += dot(latent, proj_grad.astype(jnp.bfloat16), 0, 0)

    if last:
        patch_latent, stack, node_sent = refs[9:12]
        extra = outer.shape[0]

        @pl.when(pl.program_id(0) == pl.num_programs(0) - 1)
        def _():
            node_sent[...] = node_part[...].astype(jnp.bfloat16)
            stack[:extra, :] = outer[...].astype(jnp.bfloat16)
            stack[extra : extra + width, :] = grid_part[...].astype(jnp.bfloat16)
            mesh_part = dot(patch_latent[...], node_sent[...], 0, 0)
            stack[extra + width :, :] = mesh_part.astype(jnp.bfloat16)


def edges(rows_in, columns, lanes, table, w_grid, w_both, previous, patch_latent):
    rows, row_width = rows_in.shape
    nodes, width = table.shape
    extra = row_width - width
    block = row_block(rows)
    whole = lambda shape: pl.BlockSpec(shape, lambda i: (0,) * len(shape))
    shapes = ((extra, width), (width, width), (nodes, width))
    chained = previous is not None
    last = patch_latent is not None
    in_specs = [
        pl.BlockSpec((block, row_width), lambda i: (i, 0)),
        pl.BlockSpec((block, columns.shape[1]), lambda i: (i, 0)),
        pl.BlockSpec((lanes.shape[0], block), lambda i: (0, i)),
        whole(table.shape),
        whole(w_grid.shape),
        whole(w_both.shape),
    ]
    operands = [rows_in, columns, lanes, table, w_grid, w_both]
    if chained:
        in_specs += [whole(shape) for shape in shapes]
        operands += list(previous)
    out_shape = [jax.ShapeDtypeStruct(shape, jnp.float32) for shape in shapes]
    scratch = []
    if last:
        in_specs.append(whole(patch_latent.shape))
        operands.append(patch_latent)
        out_shape = [
            jax.ShapeDtypeStruct(shape, jnp.bfloat16)
            for shape in ((extra + 2 * width, width), (nodes, width))
        ]
        scratch = [pltpu.VMEM(shape, jnp.float32) for shape in shapes]
    return pl.pallas_call(
        functools.partial(edge_body, width=width, chained=chained, last=last),
        grid=(rows // block,),
        in_specs=in_specs,
        out_specs=[whole(out.shape) for out in out_shape],
        out_shape=out_shape,
        scratch_shapes=scratch,
        compiler_params=pltpu.CompilerParams(vmem_limit_bytes=56 * 1024 * 1024),
        cost_estimate=pl.CostEstimate(
            flops=2 * rows * width * (6 * nodes + 2 * width + 2 * extra),
            bytes_accessed=rows * row_width * 2 + 4 * nodes * width * 4,
            transcendentals=3 * rows * width,
        ),
        name="edges",
    )(*operands)


def total_body(parts, out):
    total = parts[0].astype(jnp.float32)
    for part in range(1, parts.shape[0]):
        total = total + parts[part].astype(jnp.float32)
    total = total.astype(jnp.bfloat16)
    for part in range(parts.shape[0]):
        out[part] = total


def total_for_all(parts):
    return pl.pallas_call(
        total_body, out_shape=jax.ShapeDtypeStruct(parts.shape, parts.dtype), name="total"
    )(parts)


def shards(grad_pred, grid_latent, mesh_latent, send_slot, edge_src, w_mesh, w_grid, w_msg, w_out):
    grid_rows, width = grid_latent.shape
    mesh_rows = mesh_latent.shape[0]
    channels = grad_pred.shape[0]
    axes = ("band", "sub")
    devices = lax.axis_size(axes)
    members = lax.axis_size("sub")
    capacity = 3 * grid_rows // devices
    total_points = grid_rows * devices
    patch_size = members * mesh_rows
    extra = -(-channels // LANES) * LANES
    step = capacity // CHUNKS
    chunk_rows = devices * step

    def exchange(blocks):
        return lax.all_to_all(blocks, axes, split_axis=0, concat_axis=0, tiled=True)

    def from_member(block, shift):
        pairs = [((to + shift) % members, to) for to in range(members)]
        return lax.ppermute(block, "sub", pairs)

    patch_latent = jnp.concatenate(
        [mesh_latent] + [from_member(mesh_latent, shift) for shift in range(1, members)]
    )
    first_node = lax.axis_index(axes) * mesh_rows
    local = (edge_src - first_node) % patch_size
    local = local.reshape(3, devices, CHUNKS, step).transpose(2, 0, 1, 3)
    local = local.reshape(CHUNKS, 3, chunk_rows)
    local_columns = local.transpose(0, 2, 1)
    w_both = jnp.pad(
        dot(w_msg, w_out, 1, 0).astype(jnp.bfloat16), ((0, 0), (0, extra - channels))
    )
    table = dot(patch_latent, w_mesh, 1, 0).astype(jnp.bfloat16)

    points = lax.axis_index(axes) * grid_rows + jnp.arange(grid_rows, dtype=jnp.int32)
    weighted = (
        latitude_weight(points, total_points)[None, :] * grad_pred.astype(jnp.float32)
    ).astype(jnp.bfloat16)
    weighted = jnp.pad(weighted, ((0, extra - channels), (0, 0)))
    target = send_slot // capacity
    rank = send_slot % capacity
    place = (rank // step) * chunk_rows + target * step + rank % step
    place = place[None, :]

    def send(chunk, after):
        packed = pack(place, grid_latent, weighted, chunk * chunk_rows, chunk_rows, after)
        arrived = exchange(packed.reshape(devices, step, width + extra))
        return arrived.reshape(chunk_rows, width + extra)

    arrived = [send(chunk, None) for chunk in range(min(2, CHUNKS))]
    sums = None
    for chunk in range(CHUNKS):
        sums = edges(
            arrived[chunk],
            local_columns[chunk],
            local[chunk],
            table,
            w_grid,
            w_both,
            sums,
            patch_latent if chunk == CHUNKS - 1 else None,
        )
        if chunk + 2 < CHUNKS:
            arrived.append(send(chunk + 2, sums[0]))
    stack, node_sent = sums

    shares = exchange(stack.reshape(devices, stack.shape[0] // devices, width))
    node_blocks = node_sent.reshape(members, mesh_rows, width)
    node_total = node_blocks[0].astype(jnp.float32)
    for shift in range(1, members):
        node_total = node_total + from_member(node_blocks[shift], -shift).astype(jnp.float32)
    mesh_proj_grad = node_total.astype(jnp.bfloat16)
    mesh_grad = dot(mesh_proj_grad, w_mesh, 1, 1).astype(jnp.bfloat16)
    totals = exchange(total_for_all(shares)).reshape(stack.shape)
    grad_scale = 1.0 / math.sqrt(3.0 * total_points)
    outer_total = totals[:channels]
    out_total = dot(w_msg, outer_total, 0, 1)
    msg_total = dot(outer_total, w_out, 0, 1)
    return (
        mesh_grad,
        totals[extra + width :].astype(jnp.float32) * grad_scale,
        totals[extra : extra + width].astype(jnp.float32) * grad_scale,
        msg_total * grad_scale,
        out_total * grad_scale,
    )


def solution(mesh):
    placed = (
        P(None, ("band", "sub")),
        P(("band", "sub"), None),
        P(("band", "sub"), None),
        P(("band", "sub")),
        P(None, ("band", "sub")),
        P(),
        P(),
        P(),
        P(),
    )
    return jax.shard_map(
        shards,
        mesh=mesh,
        in_specs=placed,
        out_specs=(P(("band", "sub"), None), P(), P(), P(), P()),
        check_vma=False,
    )
```

```python
import functools
import math

import jax
import jax.numpy as jnp
from jax import lax
from jax.experimental import pallas as pl
from jax.experimental.pallas import tpu as pltpu
from jax.sharding import PartitionSpec as P

CHUNK_ENDS = (4, 7, 9)
CHUNKS = len(CHUNK_ENDS)
LANES = 128


def latitude_weight(points, total):
    angle = jnp.pi * ((points.astype(jnp.float32) + 0.5) / total - 0.5)
    return 0.5 * jnp.pi * jnp.cos(angle)


def dot(left, right, left_dim, right_dim):
    return lax.dot_general(
        left, right, (((left_dim,), (right_dim,)), ((), ())), preferred_element_type=jnp.float32
    )


def one_hot(index, dim, size):
    shape = (index.shape[0], size) if dim == 1 else (size, index.shape[1])
    return jnp.where(lax.broadcasted_iota(jnp.int32, shape, dim) == index, 1.0, 0.0).astype(
        jnp.bfloat16
    )


def row_block(rows):
    for block in (256, 128, 64, 32, 16, 8):
        if rows % block == 0:
            return block
    return rows


def pack_body(place, latent, weighted, *rest, block, width, base):
    out = rest[-1]
    first = base + pl.program_id(0) * block
    select = one_hot(place[...] - first, 0, block)
    out[:, :width] = dot(select, latent[...], 1, 0).astype(jnp.bfloat16)
    out[:, width:] = dot(select, weighted[...], 1, 1).astype(jnp.bfloat16)


def pack(place, latent, weighted, base, rows, after):
    width = latent.shape[1]
    extra = weighted.shape[0]
    block = row_block(rows)
    whole = lambda array: pl.BlockSpec(array.shape, lambda i: (0,) * array.ndim)
    in_specs = [whole(place), whole(latent), whole(weighted)]
    operands = [place, latent, weighted]
    if after is not None:
        in_specs.append(pl.BlockSpec((8, LANES), lambda i: (0, 0)))
        operands.append(after)
    return pl.pallas_call(
        functools.partial(pack_body, block=block, width=width, base=base),
        grid=(rows // block,),
        in_specs=in_specs,
        out_specs=pl.BlockSpec((block, width + extra), lambda i: (i, 0)),
        out_shape=jax.ShapeDtypeStruct((rows, width + extra), jnp.bfloat16),
        cost_estimate=pl.CostEstimate(
            flops=2 * rows * latent.shape[0] * (width + extra),
            bytes_accessed=rows * (width + extra) * 4,
            transcendentals=0,
        ),
        name="pack",
    )(*operands)


def edge_body(*refs, width, chained, last):
    rows_in, columns, lanes, table, w_grid, w_both = refs[:6]
    sums = refs[-3:]
    outer, grid_part, node_part = sums

    @pl.when(pl.program_id(0) == 0)
    def _():
        if chained:
            for old, new in zip(refs[6:9], sums):
                new[...] = old[...]
        else:
            for new in sums:
                new[...] = jnp.zeros_like(new)

    latent = rows_in[:, :width]
    weighted = rows_in[:, width:]
    nodes = table.shape[0]
    grid_proj = dot(latent, w_grid[...], 1, 0).astype(jnp.bfloat16).astype(jnp.float32)
    act_grad = dot(weighted, w_both[...], 1, 1)
    act_sum = None
    proj_grad = None
    node_sum = None
    for corner in range(3):
        gathered = dot(one_hot(columns[:, corner : corner + 1], 1, nodes), table[...], 1, 0)
        pre = gathered + grid_proj
        sigma = 0.5 * jnp.tanh(0.5 * pre) + 0.5
        act = pre * sigma
        grad = (act_grad * (sigma + act * (1.0 - sigma))).astype(jnp.bfloat16)
        spread = dot(one_hot(lanes[corner : corner + 1, :], 0, nodes), grad, 1, 0)
        wide = grad.astype(jnp.float32)
        act_sum = act if act_sum is None else act_sum + act
        proj_grad = wide if proj_grad is None else proj_grad + wide
        node_sum = spread if node_sum is None else node_sum + spread
    node_part[...] += node_sum
    outer[...] += dot(weighted, act_sum.astype(jnp.bfloat16), 0, 0)
    grid_part[...] += dot(latent, proj_grad.astype(jnp.bfloat16), 0, 0)

    if last:
        patch_latent, stack = refs[9:11]
        node_blocks = refs[11:-3]
        extra = outer.shape[0]

        @pl.when(pl.program_id(0) == pl.num_programs(0) - 1)
        def _():
            node_sent = node_part[...].astype(jnp.bfloat16)
            size = node_blocks[0].shape[0]
            for member, block in enumerate(node_blocks):
                block[...] = node_sent[member * size : (member + 1) * size, :]
            stack[:extra, :] = outer[...].astype(jnp.bfloat16)
            stack[extra : extra + width, :] = grid_part[...].astype(jnp.bfloat16)
            mesh_part = dot(patch_latent[...], node_sent, 0, 0)
            stack[extra + width :, :] = mesh_part.astype(jnp.bfloat16)


def edges(rows_in, columns, lanes, table, w_grid, w_both, previous, patch_latent, members):
    rows, row_width = rows_in.shape
    nodes, width = table.shape
    extra = row_width - width
    block = row_block(rows)
    whole = lambda shape: pl.BlockSpec(shape, lambda i: (0,) * len(shape))
    shapes = ((extra, width), (width, width), (nodes, width))
    chained = previous is not None
    last = patch_latent is not None
    in_specs = [
        pl.BlockSpec((block, row_width), lambda i: (i, 0)),
        pl.BlockSpec((block, columns.shape[1]), lambda i: (i, 0)),
        pl.BlockSpec((lanes.shape[0], block), lambda i: (0, i)),
        whole(table.shape),
        whole(w_grid.shape),
        whole(w_both.shape),
    ]
    operands = [rows_in, columns, lanes, table, w_grid, w_both]
    if chained:
        in_specs += [whole(shape) for shape in shapes]
        operands += list(previous)
    out_shape = [jax.ShapeDtypeStruct(shape, jnp.float32) for shape in shapes]
    scratch = []
    if last:
        in_specs.append(whole(patch_latent.shape))
        operands.append(patch_latent)
        out_shape = [
            jax.ShapeDtypeStruct(shape, jnp.bfloat16)
            for shape in ((extra + 2 * width, width),) + ((nodes // members, width),) * members
        ]
        scratch = [pltpu.VMEM(shape, jnp.float32) for shape in shapes]
    return pl.pallas_call(
        functools.partial(edge_body, width=width, chained=chained, last=last),
        grid=(rows // block,),
        in_specs=in_specs,
        out_specs=[whole(out.shape) for out in out_shape],
        out_shape=out_shape,
        scratch_shapes=scratch,
        compiler_params=pltpu.CompilerParams(vmem_limit_bytes=56 * 1024 * 1024),
        cost_estimate=pl.CostEstimate(
            flops=2 * rows * width * (6 * nodes + 2 * width + 2 * extra),
            bytes_accessed=rows * row_width * 2 + 4 * nodes * width * 4,
            transcendentals=3 * rows * width,
        ),
        name="edges",
    )(*operands)


def sum_of(blocks):
    total = blocks[0].astype(jnp.float32)
    for block in blocks[1:]:
        total = total + block.astype(jnp.float32)
    return total.astype(jnp.bfloat16)


def total_body(parts, *refs):
    out, node_out = refs[-2:]
    node_out[...] = sum_of([block[...] for block in refs[:-2]])
    total = sum_of([parts[part] for part in range(parts.shape[0])])
    for part in range(parts.shape[0]):
        out[part] = total


def total_for_all(parts, node_blocks):
    node = node_blocks[0]
    return pl.pallas_call(
        total_body,
        out_shape=[
            jax.ShapeDtypeStruct(parts.shape, parts.dtype),
            jax.ShapeDtypeStruct(node.shape, node.dtype),
        ],
        name="total",
    )(parts, *node_blocks)


def shards(grad_pred, grid_latent, mesh_latent, send_slot, edge_src, w_mesh, w_grid, w_msg, w_out):
    grid_rows, width = grid_latent.shape
    mesh_rows = mesh_latent.shape[0]
    channels = grad_pred.shape[0]
    axes = ("band", "sub")
    devices = lax.axis_size(axes)
    members = lax.axis_size("sub")
    capacity = 3 * grid_rows // devices
    total_points = grid_rows * devices
    patch_size = members * mesh_rows
    extra = -(-channels // LANES) * LANES
    ends = [capacity * end // CHUNK_ENDS[-1] for end in CHUNK_ENDS]
    spans = list(zip([0] + ends[:-1], ends))

    def exchange(blocks):
        return lax.all_to_all(blocks, axes, split_axis=0, concat_axis=0, tiled=True)

    def from_member(block, shift):
        pairs = [((to + shift) % members, to) for to in range(members)]
        return lax.ppermute(block, "sub", pairs)

    patch_latent = jnp.concatenate(
        [mesh_latent] + [from_member(mesh_latent, shift) for shift in range(1, members)]
    )
    first_node = lax.axis_index(axes) * mesh_rows
    local = (edge_src - first_node) % patch_size
    local = local.reshape(3, devices, capacity)
    local = [local[:, :, start:end].reshape(3, -1) for start, end in spans]
    w_both = jnp.pad(
        dot(w_msg, w_out, 1, 0).astype(jnp.bfloat16), ((0, 0), (0, extra - channels))
    )
    table = dot(patch_latent, w_mesh, 1, 0).astype(jnp.bfloat16)

    points = lax.axis_index(axes) * grid_rows + jnp.arange(grid_rows, dtype=jnp.int32)
    padded = jnp.pad(grad_pred, ((0, extra - channels), (0, 0)))
    weighted = (
        latitude_weight(points, total_points)[None, :] * padded.astype(jnp.float32)
    ).astype(jnp.bfloat16)
    target = send_slot // capacity
    rank = send_slot % capacity
    place = None
    for start, end in reversed(spans):
        here = start * devices + target * (end - start) + rank - start
        place = here if place is None else jnp.where(rank < end, here, place)
    place = place[None, :]

    def send(chunk, after):
        start, end = spans[chunk]
        rows = devices * (end - start)
        packed = pack(place, grid_latent, weighted, start * devices, rows, after)
        arrived = exchange(packed.reshape(devices, end - start, width + extra))
        return arrived.reshape(rows, width + extra)

    arrived = [send(chunk, None) for chunk in range(min(2, CHUNKS))]
    sums = None
    for chunk in range(CHUNKS):
        sums = edges(
            arrived[chunk],
            local[chunk].T,
            local[chunk],
            table,
            w_grid,
            w_both,
            sums,
            patch_latent if chunk == CHUNKS - 1 else None,
            members,
        )
        if chunk + 2 < CHUNKS:
            arrived.append(send(chunk + 2, sums[0]))
    stack, *node_blocks = sums

    node_blocks = [node_blocks[0]] + [
        from_member(node_blocks[shift], -shift) for shift in range(1, members)
    ]
    shares = exchange(stack.reshape(devices, stack.shape[0] // devices, width))
    totals, mesh_proj_grad = total_for_all(shares, node_blocks)
    mesh_grad = dot(mesh_proj_grad, w_mesh, 1, 1).astype(jnp.bfloat16)
    totals = exchange(totals).reshape(stack.shape)
    grad_scale = 1.0 / math.sqrt(3.0 * total_points)
    outer_total = totals[:channels]
    out_total = dot(w_msg, outer_total, 0, 1)
    msg_total = dot(outer_total, w_out, 0, 1)
    return (
        mesh_grad,
        totals[extra + width :].astype(jnp.float32) * grad_scale,
        totals[extra : extra + width].astype(jnp.float32) * grad_scale,
        msg_total * grad_scale,
        out_total * grad_scale,
    )


def solution(mesh):
    placed = (
        P(None, ("band", "sub")),
        P(("band", "sub"), None),
        P(("band", "sub"), None),
        P(("band", "sub")),
        P(None, ("band", "sub")),
        P(),
        P(),
        P(),
        P(),
    )
    return jax.shard_map(
        shards,
        mesh=mesh,
        in_specs=placed,
        out_specs=(P(("band", "sub"), None), P(), P(), P(), P()),
        check_vma=False,
    )
```
